32 devices in a mesh: dp: 8 (over y, x, core), mp: 4 (over z).
Axes of the slice: x: 2, y: 2, z: 4, core: 2. Of those that a mesh axis runs over, the one named last changes fastest.
Arguments:
- tokens: bfloat16 [8192, 2048], P('dp'), may hold values from -6 to 6
- doc_ids: int32 [16, 512], P('dp'), may hold values from 0 to 3, never falling along the last dimension, each value on 1 to 256 neighbouring positions
- selection: int32 [16, 512], P('dp'), may hold values 0 or 1
- w_query: bfloat16 [2048, 2048], P('dp', 'mp'), may hold values from -0.125 to 0.125
- w_key: bfloat16 [2048, 256], P('dp', 'mp'), may hold values from -0.125 to 0.125
- w_value: bfloat16 [2048, 256], P('dp', 'mp'), may hold values from -0.125 to 0.125
- w_out: bfloat16 [2048, 2048], P('mp', 'dp'), may hold values from -0.375 to 0.375
- w_gate: bfloat16 [2048, 5632], P('dp', 'mp'), may hold values from -0.125 to 0.125
- w_up: bfloat16 [2048, 5632], P('dp', 'mp'), may hold values from -0.125 to 0.125
- w_down: bfloat16 [5632, 2048], P('mp', 'dp'), may hold values from -0.078125 to 0.078125
- attn_gain: bfloat16 [2048], P('dp'), may hold values from 0.25 to 1.75
- mlp_gain: bfloat16 [2048], P('dp'), may hold values from 0.25 to 1.75
- cotangent: bfloat16 [8192, 2048], P('dp'), may hold values from -6 to 6
Outputs:
- output: bfloat16 [8192, 2048], P('dp')
- input_grad: float32 [8192, 2048], P('dp')
- grad_w_query: float32 [2048, 2048], P('dp', 'mp')
- grad_w_key: float32 [2048, 256], P('dp', 'mp')
- grad_w_value: float32 [2048, 256], P('dp', 'mp')
- grad_w_out: float32 [2048, 2048], P('mp', 'dp')
- grad_w_gate: float32 [2048, 5632], P('dp', 'mp')
- grad_w_up: float32 [2048, 5632], P('dp', 'mp')
- grad_w_down: float32 [5632, 2048], P('mp', 'dp')
- grad_attn_gain: float32 [2048], P('dp')
- grad_mlp_gain: float32 [2048], P('dp')
The draws below stay inside these ranges and needn't reach their ends.
Inputs may be any that keep to these rules, and one draw needn't show every extreme that they name: `doc_ids`: within a sequence the ids never fall; a document spans 1 to 256 tokens and one spans exactly 256.
All inputs are finite; a program needn't handle non-finite values. No bound on the sum of `selection` on one device may be relied on, other than what follows from the above.
Results may differ from the reference program's by a relative error of at most 0.024.
Values may be sent and summed in bfloat16 or wider, within the bound.
A program may use at most 256 MiB of HBM per device.

```python
import math
from functools import partial
import jax
import jax.numpy as jnp
import numpy as np
from jax import lax

D = 2048
HEADS = 32
KV_HEADS = 4
HEAD_DIM = 64
FF = 5632
SEQ = 512
DOCS = 4
DOC_MOST = 256
SEQS = 16
TOKENS = 8192


def place_ends(drawn, key, smallest, top_value):
    place = [jax.random.randint(jax.random.fold_in(key, axis), (), 0, length) for axis, length in enumerate(drawn.shape)]
    widest = drawn.shape.index(max(drawn.shape))
    beside = place[:widest] + [(place[widest] + 1) % drawn.shape[widest]] + place[widest + 1:]
    return drawn.at[tuple(place)].set(smallest).at[tuple(beside)].set(top_value)


def raised(entries, key, source, target, parts, factor):
    def block_of(dim):
        return (jnp.arange(entries.shape[dim]) // (entries.shape[dim] // parts)).reshape((-1,) + (1,) * (entries.ndim - 1 - dim))

    near = jax.random.permutation(key, parts)[block_of(target)]
    second = (block_of(target) + parts // 2) % parts
    return jnp.where((block_of(source) == near) | (block_of(source) == second), factor * entries, entries)


def block_scale(rng, extent, split, smallest, high):
    level, own = 1.0, jax.random.fold_in(rng, 6)
    for axis_at, parts in split:
        heights = jnp.exp(jax.random.uniform(jax.random.fold_in(own, axis_at), (parts,), jnp.float32, smallest / len(split), high / len(split)))
        level = level * jnp.repeat(heights, extent[axis_at] // parts).reshape([-1 if axis == axis_at else 1 for axis in range(len(extent))])
    return level


def profile(number_of, total, reach, lean):
    portions = [(1 << 20) // math.isqrt(grade ** lean) + 1 for grade in range(2, number_of + 1)]
    rest, holding = total - reach - (number_of - 1), [1] * (number_of - 1)
    while rest > 0:
        candidates = [i for i in range(number_of - 1) if holding[i] < reach]
        whole, budget = sum([portions[i] for i in candidates]), rest
        for i in candidates:
            extra = min(reach - holding[i], max(1, budget * portions[i] // whole), rest)
            holding[i] = holding[i] + extra
            rest = rest - extra
    return np.array([reach] + holding)


def uneven_parts(rng, count, total, most, slope):
    if count == 2:
        one = jax.random.randint(rng, (), max(1, total - most), min(most, total - 1) + 1)
        return jnp.stack([one, total - one])
    sizes = jnp.asarray(profile(count, total, most, slope), jnp.int32)
    couples = (count - 1) // 2
    donor, sink = sizes[1:1 + 2 * couples:2], sizes[2:2 + 2 * couples:2]
    margin = jnp.minimum(donor - 1, most - sink)
    shifted = jax.random.randint(jax.random.fold_in(rng, 1), (couples,), 0, 1 << 20) % (margin + 1)
    sizes = sizes.at[1:1 + 2 * couples:2].set(donor - shifted).at[2:2 + 2 * couples:2].set(sink + shifted)
    return sizes[jax.random.permutation(jax.random.fold_in(rng, 2), count)]


def scatter_about(own_key, extent, deviation, bound, cuts=(), kind=jnp.bfloat16):
    array = deviation * jax.random.normal(own_key, extent, jnp.float32)
    if cuts:
        array = array * block_scale(own_key, extent, cuts, -0.22, 0.18)
    return jnp.clip(array, -bound, bound).astype(kind)


def gaussian_with(rng, extent, scale, bound, cuts, heavy, kind=jnp.bfloat16):
    values = scale * jax.random.normal(rng, extent, jnp.float32)
    if cuts:
        values = values * block_scale(rng, extent, cuts, -0.22, 0.18)
    return jnp.clip(raised(values, jax.random.fold_in(rng, 3), *heavy), -bound, bound).astype(kind)


def setup_inputs(seed: int = 0) -> dict:
    keys = jax.random.split(jax.random.key(seed), 14)
    return {
        "tokens": gaussian_with(keys[0], (TOKENS, D), 1.0, 6.0, ((0, 8),), (0, 1, 8, 2.0)),
        "doc_ids": jax.vmap(lambda own: jnp.searchsorted(jnp.cumsum(uneven_parts(own, DOCS, SEQ, DOC_MOST, 0)), jnp.arange(SEQ), side="right"))(jax.random.split(keys[1], SEQS)).reshape((SEQS, SEQ)).astype(jnp.int32),
        "selection": place_ends((jax.random.randint(keys[2], (SEQS, SEQ), 0, 5) < 3).astype(jnp.int32), jax.random.fold_in(keys[2], 1), 0, 1),
        "w_query": scatter_about(keys[3], (D, HEADS * HEAD_DIM), D ** -0.5, 0.125, ((0, 8), (1, 4))),
        "w_key": scatter_about(keys[4], (D, KV_HEADS * HEAD_DIM), D ** -0.5, 0.125, ((0, 8), (1, 4))),
        "w_value": scatter_about(keys[5], (D, KV_HEADS * HEAD_DIM), D ** -0.5, 0.125, ((0, 8), (1, 4))),
        "w_out": scatter_about(keys[6], (HEADS * HEAD_DIM, D), (D // 8) ** -0.5, 0.375, ((0, 4), (1, 8))),
        "w_gate": scatter_about(keys[7], (D, FF), D ** -0.5, 0.125, ((0, 8), (1, 4))),
        "w_up": scatter_about(keys[8], (D, FF), D ** -0.5, 0.125, ((0, 8), (1, 4))),
        "w_down": scatter_about(keys[9], (FF, D), FF ** -0.5, 0.078125, ((0, 4), (1, 8))),
        "attn_gain": jnp.clip(1.0 + 0.15 * jax.random.normal(keys[10], (D,), jnp.float32), 0.25, 1.75).astype(jnp.bfloat16),
        "mlp_gain": jnp.clip(1.0 + 0.15 * jax.random.normal(keys[11], (D,), jnp.float32), 0.25, 1.75).astype(jnp.bfloat16),
        "cotangent": gaussian_with(keys[12], (TOKENS, D), 1.0, 6.0, ((0, 8),), (0, 1, 8, 2.0)),
    }


EPSILON = 1e-05
MASKED = -1e+30
HIGH = lax.Precision.HIGHEST

@jax.custom_vjp
def low(v):
    return lax.optimization_barrier(v.astype(jnp.bfloat16)).astype(jnp.float32)

@jax.custom_vjp
def low_back(v):
    return v

def low_keep(v):
    return (low(v), None)

def low_pass(kept, grad):
    return (grad,)

def back_keep(v):
    return (v, None)

def back_low(kept, grad):
    return (low(grad),)
low.defvjp(low_keep, low_pass)
low_back.defvjp(back_keep, back_low)

def rope_tables(length, head_width):
    half_width = head_width // 2
    frequency = 10000.0 ** (-2.0 * jnp.arange(half_width, dtype=jnp.float32) / head_width)
    places = jnp.arange(length, dtype=jnp.float32)
    angles = places[:, None] * frequency[None, :]
    return (jnp.cos(angles)[:, None, :], jnp.sin(angles)[:, None, :])

def rotate(field, cosine_table, sine_table):
    half_width = field.shape[-1] // 2
    first_half = field[..., :half_width]
    second_half = field[..., half_width:]
    return jnp.concatenate([first_half * cosine_table - second_half * sine_table, second_half * cosine_table + first_half * sine_table], axis=-1)

def allowed_pairs(doc_row):
    length = doc_row.shape[0]
    query_index = lax.broadcasted_iota(jnp.int32, (length, length), 0)
    key_index = lax.broadcasted_iota(jnp.int32, (length, length), 1)
    return (doc_row[:, None] == doc_row[None, :]) & (query_index >= key_index)

def rms_scale(residual, gain_row):
    inverse = lax.rsqrt(lax.optimization_barrier(jnp.mean(residual * residual, axis=-1, keepdims=True)) + EPSILON)
    return residual * inverse * gain_row

def attend_bundle(bundle):
    queries, key_rows, value_rows, doc_row = bundle
    length = doc_row.shape[0]
    grouped = queries.reshape(length, KV_HEADS, HEADS // KV_HEADS, HEAD_DIM)
    scores = low_back(HEAD_DIM ** (-0.5) * jnp.einsum('qkgd,skd->kgqs', grouped, key_rows, precision=HIGH))
    scores = jnp.where(allowed_pairs(doc_row), scores, MASKED)
    highest = lax.optimization_barrier(jnp.max(scores, axis=-1, keepdims=True))
    shifted_exp = jnp.exp(scores - highest)
    attn_probs = low(shifted_exp / lax.optimization_barrier(jnp.sum(shifted_exp, axis=-1, keepdims=True)))
    mixed_heads = jnp.einsum('kgqs,skd->qkgd', attn_probs, value_rows, precision=HIGH)
    return mixed_heads.reshape(length, HEADS * HEAD_DIM)

def forward(tokens, w_query, w_key, w_value, w_out, w_gate, w_up, w_down, attn_gain, mlp_gain, doc_ids):
    seq_count, length = doc_ids.shape
    cosine_table, sine_table = rope_tables(length, HEAD_DIM)
    normed_one = low(rms_scale(tokens, attn_gain))
    query_lin = low_back(jnp.dot(normed_one, w_query, precision=HIGH)).reshape(seq_count, length, HEADS, HEAD_DIM)
    key_lin = low_back(jnp.dot(normed_one, w_key, precision=HIGH)).reshape(seq_count, length, KV_HEADS, HEAD_DIM)
    value_rows = low(low_back(jnp.dot(normed_one, w_value, precision=HIGH))).reshape(seq_count, length, KV_HEADS, HEAD_DIM)
    query_rot = low(rotate(query_lin, cosine_table, sine_table))
    key_rot = low(rotate(key_lin, cosine_table, sine_table))
    mixed_heads = lax.map(jax.checkpoint(attend_bundle), (query_rot, key_rot, value_rows, doc_ids))
    mixed_low = low(low_back(mixed_heads.reshape(seq_count * length, HEADS * HEAD_DIM)))
    attn_out = low_back(jnp.dot(mixed_low, w_out, precision=HIGH))
    hidden_in = tokens + attn_out
    normed_two = low(rms_scale(hidden_in, mlp_gain))
    gate_lin = low_back(jnp.dot(normed_two, w_gate, precision=HIGH))
    up_lin = low_back(jnp.dot(normed_two, w_up, precision=HIGH))
    hidden = low(gate_lin * jax.nn.sigmoid(gate_lin) * up_lin)
    mlp_out = low_back(jnp.dot(hidden, w_down, precision=HIGH))
    return hidden_in + mlp_out

def reference(tokens, doc_ids, selection, w_query, w_key, w_value, w_out, w_gate, w_up, w_down, attn_gain, mlp_gain, cotangent):
    result, pullback = jax.vjp(partial(forward, doc_ids=doc_ids), tokens.astype(jnp.float32), w_query.astype(jnp.float32), w_key.astype(jnp.float32), w_value.astype(jnp.float32), w_out.astype(jnp.float32), w_gate.astype(jnp.float32), w_up.astype(jnp.float32), w_down.astype(jnp.float32), attn_gain.astype(jnp.float32), mlp_gain.astype(jnp.float32))
    token_weight = selection.reshape(-1, 1).astype(jnp.float32)
    grads = pullback(cotangent.astype(jnp.float32) * token_weight)
    return (result.astype(jnp.bfloat16), grads[0], grads[1], grads[2], grads[3], grads[4], grads[5], grads[6], grads[7], grads[8], grads[9])
```

```python
import jax
import jax.numpy as jnp
from jax import lax
from jax.experimental import pallas as pl
from jax.experimental.pallas import tpu as pltpu
from jax.sharding import PartitionSpec as P

HEAD_DIM = 64
LANES = 128
EPSILON = 1e-05
MASKED = -1e30
QBLOCK = 128
REACH = 256
F32 = jnp.float32
BF16 = jnp.bfloat16

INWARD = [(0, 1), (3, 2)]
ACROSS = [(1, 2), (2, 1)]
OUTWARD = [(1, 0), (2, 3)]


def rope_tables(length):
    half_width = HEAD_DIM // 2
    frequency = 10000.0 ** (-2.0 * jnp.arange(half_width, dtype=F32) / HEAD_DIM)
    places = jnp.arange(length, dtype=F32)
    angles = places[:, None] * frequency[None, :]
    cosine, sine = jnp.cos(angles), jnp.sin(angles)
    return (
        jnp.concatenate([cosine] * 4, axis=1),
        jnp.concatenate([-sine, sine] * 2, axis=1),
    )


def nt(a, b):
    return lax.dot_general(a, b, (((1,), (1,)), ((), ())), preferred_element_type=F32)


def tn(a, b):
    return lax.dot_general(a, b, (((0,), (0,)), ((), ())), preferred_element_type=F32)


def nn(a, b):
    return lax.dot_general(a, b, (((1,), (0,)), ((), ())), preferred_element_type=F32)


def swap_halves(block, lane):
    ahead = pltpu.roll(block, LANES - HEAD_DIM // 2, 1)
    behind = pltpu.roll(block, HEAD_DIM // 2, 1)
    return jnp.where(lane % HEAD_DIM < HEAD_DIM // 2, ahead, behind)


def turn(block, cosine, sine, lane):
    return block * cosine + swap_halves(block, lane) * sine


def key_range(q):
    start = max(0, q * QBLOCK - REACH)
    return start, (q + 1) * QBLOCK - start


def pair_bias(doc_col, doc_row, q):
    start, count = key_range(q)
    rows = lax.broadcasted_iota(jnp.int32, (QBLOCK, count), 0) + q * QBLOCK
    cols = lax.broadcasted_iota(jnp.int32, (QBLOCK, count), 1) + start
    same = doc_col[q * QBLOCK : (q + 1) * QBLOCK, 0:1] == doc_row[0:1, start : start + count]
    return jnp.where(same & (rows >= cols), 0.0, MASKED)


def attend_forward_kernel(
    scale, q_ref, kv_ref, doc_col, doc_row, cos_ref, sin_ref, mixed_ref, rot_ref, kvr_ref, lse_ref, spread
):
    length = q_ref.shape[0]
    j = pl.program_id(0)
    lane = lax.broadcasted_iota(jnp.int32, (length, LANES), 1)

    @pl.when(j == 0)
    def _():
        kv = kv_ref[...]
        turned = turn(kv, cos_ref[...], sin_ref[...], lane)
        kvr_ref[...] = jnp.where(lane < HEAD_DIM, turned, kv).astype(BF16)
        low_key = jnp.where(lane < HEAD_DIM, turned, 0.0)
        high_value = jnp.where(lane < HEAD_DIM, 0.0, kv)
        spread[0] = low_key.astype(BF16)
        spread[1] = pltpu.roll(low_key, HEAD_DIM, 1).astype(BF16)
        spread[2] = pltpu.roll(high_value, HEAD_DIM, 1).astype(BF16)
        spread[3] = high_value.astype(BF16)
        lse_ref[...] = jnp.zeros_like(lse_ref)

    rot = turn(q_ref[...], cos_ref[...], sin_ref[...], lane).astype(BF16)
    rot_ref[...] = rot
    for q in range(length // QBLOCK):
        start, count = key_range(q)
        rows = slice(q * QBLOCK, (q + 1) * QBLOCK)
        keys = slice(start, start + count)
        bias = pair_bias(doc_col, doc_row, q)
        mixed = jnp.zeros((QBLOCK, LANES), F32)
        for half in range(2):
            scores = nt(rot[rows], spread[half, keys]) * scale + bias
            highest = jnp.max(scores, axis=1, keepdims=True)
            raised = jnp.exp(scores - highest)
            total = jnp.sum(raised, axis=1, keepdims=True)
            probs = (raised * (1.0 / total)).astype(BF16)
            mixed = mixed + nn(probs, spread[2 + half, keys])
            lse_ref[rows] = jnp.where(
                lane[rows] == 2 * j + half, highest + jnp.log(total), lse_ref[rows]
            )
        mixed_ref[rows] = mixed.astype(BF16)


def attend_backward_kernel(
    scale, pairs, rot_ref, kvr_ref, gm_ref, lse_ref, doc_col, doc_row, cos_ref, sin_ref, out_ref, spread, dkey, dvalue
):
    length = rot_ref.shape[0]
    j = pl.program_id(0)
    lane = lax.broadcasted_iota(jnp.int32, (length, LANES), 1)

    @pl.when(j == 0)
    def _():
        kvr = kvr_ref[...].astype(F32)
        low_key = jnp.where(lane < HEAD_DIM, kvr, 0.0)
        high_value = jnp.where(lane < HEAD_DIM, 0.0, kvr)
        spread[0] = low_key.astype(BF16)
        spread[1] = pltpu.roll(low_key, HEAD_DIM, 1).astype(BF16)
        spread[2] = pltpu.roll(high_value, HEAD_DIM, 1).astype(BF16)
        spread[3] = high_value.astype(BF16)
        dkey[...] = jnp.zeros_like(dkey)
        dvalue[...] = jnp.zeros_like(dvalue)

    @pl.when(j < pairs)
    def _():
        for q in range(length // QBLOCK):
            start, count = key_range(q)
            rows = slice(q * QBLOCK, (q + 1) * QBLOCK)
            keys = slice(start, start + count)
            bias = pair_bias(doc_col, doc_row, q)
            rot, gm = rot_ref[rows], gm_ref[rows]
            dquery = jnp.zeros((QBLOCK, LANES), F32)
            for half in range(2):
                logsum = jnp.sum(
                    jnp.where(lane[rows] == 2 * j + half, lse_ref[rows], 0.0), axis=1, keepdims=True
                )
                scores = nt(rot, spread[half, keys]) * scale + bias
                probs = jnp.exp(scores - logsum)
                dprobs = nt(gm, spread[2 + half, keys])
                inner = jnp.sum(probs * dprobs, axis=1, keepdims=True)
                dscores = (probs * (dprobs - inner)).astype(BF16)
                dquery = dquery + nn(dscores, spread[half, keys])
                dkey[half, keys] += tn(dscores, rot)
                dvalue[half, keys] += tn(probs.astype(BF16), gm)
            out_ref[rows] = turn(dquery * scale, cos_ref[rows], -sin_ref[rows], lane[rows]).astype(BF16)

    @pl.when(j == pairs)
    def _():
        dk = dkey[0] + pltpu.roll(dkey[1], HEAD_DIM, 1)
        dv = pltpu.roll(dvalue[0], HEAD_DIM, 1) + dvalue[1]
        back = turn(dk * scale, cos_ref[...], -sin_ref[...], lane)
        out_ref[...] = jnp.where(lane < HEAD_DIM, back, dv).astype(BF16)


def whole(shape):
    return pl.BlockSpec(shape, lambda j: (0,) * len(shape))


def attend_forward(qkv, doc, cosine, sine, heads):
    length = doc.shape[0]
    pairs = heads * HEAD_DIM // LANES
    column = pl.BlockSpec((length, LANES), lambda j: (0, j))
    return pl.pallas_call(
        lambda *refs: attend_forward_kernel(HEAD_DIM ** (-0.5), *refs),
        grid=(pairs,),
        in_specs=[
            column,
            pl.BlockSpec((length, LANES), lambda j: (0, pairs)),
            whole((length, 1)),
            whole((1, length)),
            whole((length, LANES)),
            whole((length, LANES)),
        ],
        out_specs=[column, column, whole((length, LANES)), whole((length, LANES))],
        out_shape=[
            jax.ShapeDtypeStruct((length, pairs * LANES), BF16),
            jax.ShapeDtypeStruct((length, pairs * LANES), BF16),
            jax.ShapeDtypeStruct((length, LANES), BF16),
            jax.ShapeDtypeStruct((length, LANES), F32),
        ],
        scratch_shapes=[pltpu.VMEM((4, length, LANES), BF16)],
        cost_estimate=pl.CostEstimate(flops=600_000_000, bytes_accessed=4_000_000, transcendentals=1_200_000),
        name="attend_forward",
    )(qkv, qkv, doc.reshape(length, 1), doc.reshape(1, length), cosine, sine)


def attend_backward(rot, kvr, gm, lse, doc, cosine, sine):
    length, width = rot.shape
    pairs = width // LANES
    column = pl.BlockSpec((length, LANES), lambda j: (0, jnp.minimum(j, pairs - 1)))
    return pl.pallas_call(
        lambda *refs: attend_backward_kernel(HEAD_DIM ** (-0.5), pairs, *refs),
        grid=(pairs + 1,),
        in_specs=[
            column,
            whole((length, LANES)),
            column,
            whole((length, LANES)),
            whole((length, 1)),
            whole((1, length)),
            whole((length, LANES)),
            whole((length, LANES)),
        ],
        out_specs=pl.BlockSpec((length, LANES), lambda j: (0, j)),
        out_shape=jax.ShapeDtypeStruct((length, (pairs + 1) * LANES), BF16),
        scratch_shapes=[
            pltpu.VMEM((4, length, LANES), BF16),
            pltpu.VMEM((2, length, LANES), F32),
            pltpu.VMEM((2, length, LANES), F32),
        ],
        cost_estimate=pl.CostEstimate(flops=1_500_000_000, bytes_accessed=4_000_000, transcendentals=1_200_000),
        name="attend_backward",
    )(rot, kvr, gm, lse, doc.reshape(length, 1), doc.reshape(1, length), cosine, sine)


def rms_inverse(residual):
    return lax.rsqrt(jnp.mean(residual * residual, axis=-1, keepdims=True) + EPSILON)


class Line:
    def __init__(self):
        place = lax.axis_index("mp")
        self.end = (place == 0) | (place == 3)
        self.across = self.outward = None
        self.sums = {}

    def step(self, name=None, piece=None, keep=()):
        arrived = met = back = None
        if name is not None:
            arrived = lax.ppermute(piece, "mp", INWARD)
        if self.across is not None:
            met = lax.ppermute(self.across[1], "mp", ACROSS)
        if self.outward is not None:
            back = lax.ppermute(self.outward[1], "mp", OUTWARD)
        keep, arrived, met, back = lax.optimization_barrier((keep, arrived, met, back))
        if back is not None:
            self.sums[self.outward[0]] = jnp.where(self.end, back, self.outward[1])
        self.outward = None if met is None else (self.across[0], self.across[1] + met)
        self.across = None if arrived is None else (name, piece + arrived)
        if self.outward is not None or self.across is not None:
            self.outward, self.across = self.rounded(self.outward), self.rounded(self.across)
        return keep

    def rounded(self, entry):
        return None if entry is None else (entry[0], lax.optimization_barrier(entry[1]))


def per_device(
    tokens, doc_ids, selection, w_query, w_key, w_value, w_out, w_gate, w_up, w_down,
    attn_gain, mlp_gain, cotangent,
):
    rows_local, q_width = w_query.shape
    kv_width = w_key.shape[1]
    ff = w_gate.shape[1]
    heads = q_width // HEAD_DIM
    qkv_width = q_width + 2 * kv_width
    seqs, length = doc_ids.shape
    pad = jnp.zeros((rows_local, LANES - 2), BF16)
    front = jnp.concatenate(
        [w_query, w_key, w_value, attn_gain[:, None], mlp_gain[:, None], pad], axis=1
    )
    front = lax.all_gather(front, "dp", axis=0, tiled=True)
    w_qkv = front[:, :qkv_width]
    gain_one = front[:, qkv_width].astype(F32)[None, :]
    gain_two = front[:, qkv_width + 1].astype(F32)[None, :]
    full_out = lax.all_gather(w_out, "dp", axis=1, tiled=True)
    full_gate = lax.all_gather(w_gate, "dp", axis=0, tiled=True)
    full_up = lax.all_gather(w_up, "dp", axis=0, tiled=True)
    full_down = lax.all_gather(w_down, "dp", axis=1, tiled=True)

    cosine, sine = rope_tables(length)
    residual = tokens.astype(F32)
    inverse_one = rms_inverse(residual)
    normed_one = (residual * inverse_one * gain_one).astype(BF16)
    grad_y = cotangent.astype(F32) * selection.reshape(-1, 1).astype(F32)
    grad_y_low = grad_y.astype(BF16)

    halves = range(seqs)
    span = [slice(h * length, (h + 1) * length) for h in halves]
    cut = length // 2

    def parts(array):
        return array[:cut], array[cut:]

    line = Line()

    def attention(h):
        qkv = nn(normed_one[span[h]], w_qkv)
        mixed, rot, kvr, lse = attend_forward(qkv, doc_ids[h], cosine, sine, heads)
        partial = nn(mixed, full_out).astype(BF16)
        return mixed, rot, kvr, lse, partial

    def mlp_forward(h):
        attn = jnp.concatenate([line.sums["1", h, 0], line.sums["1", h, 1]], axis=0)
        hidden_in = residual[span[h]] + attn.astype(F32)
        inverse_two = rms_inverse(hidden_in)
        normed_two = (hidden_in * inverse_two * gain_two).astype(BF16)
        gate = nn(normed_two, full_gate)
        up = nn(normed_two, full_up)
        hidden = (gate * jax.nn.sigmoid(gate) * up).astype(BF16)
        partial = nn(hidden, full_down).astype(BF16)
        return attn, normed_two, gate, up, hidden, partial

    def mlp_backward(h, gate, up):
        grad_hidden = nt(grad_y_low[span[h]], full_down)
        sig = jax.nn.sigmoid(gate)
        grad_gate = (grad_hidden * up * sig * (1.0 + gate * (1.0 - sig))).astype(BF16)
        grad_up = (grad_hidden * gate * sig).astype(BF16)
        partial = (nt(grad_gate, full_gate) + nt(grad_up, full_up)).astype(BF16)
        return grad_gate, grad_up, partial

    def attention_backward(h, saved, attn):
        mixed, rot, kvr, lse = saved
        hidden_in = residual[span[h]] + attn.astype(F32)
        inverse_two = rms_inverse(hidden_in)
        grad_normed = jnp.concatenate([line.sums["3", h, 0], line.sums["3", h, 1]], axis=0).astype(F32)
        scaled = grad_normed * gain_two
        gain_part = jnp.sum(grad_normed * hidden_in * inverse_two, axis=0)
        mean_term = jnp.mean(scaled * hidden_in, axis=-1, keepdims=True)
        grad_h = (
            grad_y[span[h]] + inverse_two * scaled - hidden_in * (inverse_two**3) * mean_term
        )
        grad_h_low = grad_h.astype(BF16)
        grad_mixed = nt(grad_h_low, full_out).astype(BF16)
        grad_qkv = attend_backward(rot, kvr, grad_mixed, lse, doc_ids[h], cosine, sine)
        partial = nt(grad_qkv, w_qkv).astype(BF16)
        return grad_h, grad_h_low, grad_qkv, partial, gain_part

    def finish(h, grad_h):
        grad_normed = jnp.concatenate([line.sums["4", h, 0], line.sums["4", h, 1]], axis=0).astype(F32)
        here, inverse = residual[span[h]], inverse_one[span[h]]
        scaled = grad_normed * gain_one
        gain_part = jnp.sum(grad_normed * here * inverse, axis=0)
        mean_term = jnp.mean(scaled * here, axis=-1, keepdims=True)
        return grad_h + inverse * scaled - here * (inverse**3) * mean_term, gain_part

    def scatter(grad, axis):
        return lax.psum_scatter(grad.astype(BF16), "dp", scatter_dimension=axis, tiled=True).astype(F32)

    a = attention(0)
    a_parts = parts(a[4])
    (b,) = line.step(("1", 0, 0), a_parts[0], (attention(1),))
    b_parts = parts(b[4])
    line.step(("1", 0, 1), a_parts[1])
    line.step(("1", 1, 0), b_parts[0])
    line.step(("1", 1, 1), b_parts[1])
    (fa,) = line.step(keep=(mlp_forward(0),))
    attn_a, normed_a, gate_a, up_a, hidden_a, out_a = fa
    out_a = parts(out_a)
    (ba,) = line.step(("2", 0, 0), out_a[0], (mlp_backward(0, gate_a, up_a),))
    gg_a, gu_a, dn_a = ba
    dn_a = parts(dn_a)
    (fb,) = line.step(("3", 0, 0), dn_a[0], (mlp_forward(1),))
    attn_b, normed_b, gate_b, up_b, hidden_b, out_b = fb
    out_b = parts(out_b)
    (bb,) = line.step(("3", 0, 1), dn_a[1], (mlp_backward(1, gate_b, up_b),))
    gg_b, gu_b, dn_b = bb
    dn_b = parts(dn_b)

    def both(first, second):
        return jnp.concatenate([first, second], axis=0)

    normed_two = both(normed_a, normed_b)
    (grad_gate_w, grad_up_w) = line.step(
        ("3", 1, 0),
        dn_b[0],
        (tn(normed_two, both(gg_a, gg_b)).astype(BF16), tn(normed_two, both(gu_a, gu_b)).astype(BF16)),
    )
    (grad_down_w,) = line.step(
        ("3", 1, 1), dn_b[1], (tn(both(hidden_a, hidden_b), grad_y_low).astype(BF16),)
    )
    (ca,) = line.step(("2", 0, 1), out_a[1], (attention_backward(0, a[:4], attn_a),))
    gh_a, ghl_a, gq_a, dx_a, gain_two_a = ca
    dx_a = parts(dx_a)
    line.step(("4", 0, 0), dx_a[0])
    (cb,) = line.step(("4", 0, 1), dx_a[1], (attention_backward(1, b[:4], attn_b),))
    gh_b, ghl_b, gq_b, dx_b, gain_two_b = cb
    dx_b = parts(dx_b)
    grad_qkv_w, grad_out_w = line.step(
        ("4", 1, 0),
        dx_b[0],
        (
            tn(normed_one, both(gq_a, gq_b)).astype(BF16),
            tn(both(a[0], b[0]), both(ghl_a, ghl_b)).astype(BF16),
        ),
    )
    line.step(("4", 1, 1), dx_b[1])
    (da,) = line.step(("2", 1, 0), out_b[0], (finish(0, gh_a),))
    line.step(("2", 1, 1), out_b[1])
    (db,) = line.step(keep=(finish(1, gh_b),))
    line.step()

    input_grad = both(da[0], db[0])
    hidden_in = residual + both(attn_a, attn_b).astype(F32)
    mlp_out = jnp.concatenate([line.sums["2", h, i] for h in halves for i in range(2)], axis=0)
    output = (hidden_in + mlp_out.astype(F32)).astype(BF16)
    shard_qkv = scatter(grad_qkv_w, 0)
    return (
        output,
        input_grad,
        shard_qkv[:, :q_width],
        shard_qkv[:, q_width : q_width + kv_width],
        shard_qkv[:, q_width + kv_width :],
        scatter(grad_out_w, 1),
        scatter(grad_gate_w, 0),
        scatter(grad_up_w, 0),
        scatter(grad_down_w, 1),
        scatter(da[1] + db[1], 0),
        scatter(gain_two_a + gain_two_b, 0),
    )


def solution(mesh):
    in_specs = (
        P("dp", None), P("dp", None), P("dp", None), P("dp", "mp"), P("dp", "mp"), P("dp", "mp"),
        P("mp", "dp"), P("dp", "mp"), P("dp", "mp"), P("mp", "dp"), P("dp"), P("dp"), P("dp", None),
    )
    out_specs = (
        P("dp", None), P("dp", None), P("dp", "mp"), P("dp", "mp"), P("dp", "mp"), P("mp", "dp"),
        P("dp", "mp"), P("dp", "mp"), P("mp", "dp"), P("dp"), P("dp"),
    )
    return jax.shard_map(
        per_device, mesh=mesh, in_specs=in_specs, out_specs=out_specs, check_vma=False
    )
```

```python
import jax
import jax.numpy as jnp
from jax import lax
from jax.experimental import pallas as pl
from jax.experimental.pallas import tpu as pltpu
from jax.sharding import PartitionSpec as P

HEAD_DIM = 64
LANES = 128
EPSILON = 1e-05
MASKED = -1e30
QBLOCK = 128
REACH = 256
F32 = jnp.float32
BF16 = jnp.bfloat16

INWARD = [(0, 1), (3, 2)]
ACROSS = [(1, 2), (2, 1)]
OUTWARD = [(1, 0), (2, 3)]


def rope_tables(length):
    half_width = HEAD_DIM // 2
    frequency = 10000.0 ** (-2.0 * jnp.arange(half_width, dtype=F32) / HEAD_DIM)
    places = jnp.arange(length, dtype=F32)
    angles = places[:, None] * frequency[None, :]
    cosine, sine = jnp.cos(angles), jnp.sin(angles)
    return (
        jnp.concatenate([cosine] * 4, axis=1),
        jnp.concatenate([-sine, sine] * 2, axis=1),
    )


def nt(a, b):
    return lax.dot_general(a, b, (((1,), (1,)), ((), ())), preferred_element_type=F32)


def tn(a, b):
    return lax.dot_general(a, b, (((0,), (0,)), ((), ())), preferred_element_type=F32)


def nn(a, b):
    return lax.dot_general(a, b, (((1,), (0,)), ((), ())), preferred_element_type=F32)


def swap_halves(block, lane):
    ahead = pltpu.roll(block, LANES - HEAD_DIM // 2, 1)
    behind = pltpu.roll(block, HEAD_DIM // 2, 1)
    return jnp.where(lane % HEAD_DIM < HEAD_DIM // 2, ahead, behind)


def turn(block, cosine, sine, lane):
    return block * cosine + swap_halves(block, lane) * sine


def key_range(q):
    start = max(0, q * QBLOCK - REACH)
    return start, (q + 1) * QBLOCK - start


def pair_bias(doc_col, doc_row, q):
    start, count = key_range(q)
    rows = lax.broadcasted_iota(jnp.int32, (QBLOCK, count), 0) + q * QBLOCK
    cols = lax.broadcasted_iota(jnp.int32, (QBLOCK, count), 1) + start
    same = doc_col[q * QBLOCK : (q + 1) * QBLOCK, 0:1] == doc_row[0:1, start : start + count]
    return jnp.where(same & (rows >= cols), 0.0, MASKED)


def attend_forward_kernel(
    scale, q_ref, kv_ref, doc_col, doc_row, cos_ref, sin_ref, mixed_ref, rot_ref, kvr_ref, lse_ref, spread
):
    length = q_ref.shape[0]
    j = pl.program_id(0)
    lane = lax.broadcasted_iota(jnp.int32, (length, LANES), 1)

    @pl.when(j == 0)
    def _():
        kv = kv_ref[...]
        turned = turn(kv, cos_ref[...], sin_ref[...], lane)
        kvr_ref[...] = jnp.where(lane < HEAD_DIM, turned, kv).astype(BF16)
        low_key = jnp.where(lane < HEAD_DIM, turned, 0.0)
        high_value = jnp.where(lane < HEAD_DIM, 0.0, kv)
        spread[0] = low_key.astype(BF16)
        spread[1] = pltpu.roll(low_key, HEAD_DIM, 1).astype(BF16)
        spread[2] = pltpu.roll(high_value, HEAD_DIM, 1).astype(BF16)
        spread[3] = high_value.astype(BF16)
        lse_ref[...] = jnp.zeros_like(lse_ref)

    rot = turn(q_ref[...], cos_ref[...], sin_ref[...], lane).astype(BF16)
    rot_ref[...] = rot
    for q in range(length // QBLOCK):
        start, count = key_range(q)
        rows = slice(q * QBLOCK, (q + 1) * QBLOCK)
        keys = slice(start, start + count)
        bias = pair_bias(doc_col, doc_row, q)
        mixed = jnp.zeros((QBLOCK, LANES), F32)
        for half in range(2):
            scores = nt(rot[rows], spread[half, keys]) * scale + bias
            highest = jnp.max(scores, axis=1, keepdims=True)
            raised = jnp.exp(scores - highest)
            total = jnp.sum(raised, axis=1, keepdims=True)
            probs = (raised * (1.0 / total)).astype(BF16)
            mixed = mixed + nn(probs, spread[2 + half, keys])
            lse_ref[rows] = jnp.where(
                lane[rows] == 2 * j + half, highest + jnp.log(total), lse_ref[rows]
            )
        mixed_ref[rows] = mixed.astype(BF16)


def attend_backward_kernel(
    scale, pairs, rot_ref, kvr_ref, gm_ref, lse_ref, doc_col, doc_row, cos_ref, sin_ref, out_ref, spread, dkey, dvalue
):
    length = rot_ref.shape[0]
    j = pl.program_id(0)
    lane = lax.broadcasted_iota(jnp.int32, (length, LANES), 1)

    @pl.when(j == 0)
    def _():
        kvr = kvr_ref[...].astype(F32)
        low_key = jnp.where(lane < HEAD_DIM, kvr, 0.0)
        high_value = jnp.where(lane < HEAD_DIM, 0.0, kvr)
        spread[0] = low_key.astype(BF16)
        spread[1] = pltpu.roll(low_key, HEAD_DIM, 1).astype(BF16)
        spread[2] = pltpu.roll(high_value, HEAD_DIM, 1).astype(BF16)
        spread[3] = high_value.astype(BF16)
        dkey[...] = jnp.zeros_like(dkey)
        dvalue[...] = jnp.zeros_like(dvalue)

    @pl.when(j < pairs)
    def _():
        for q in range(length // QBLOCK):
            start, count = key_range(q)
            rows = slice(q * QBLOCK, (q + 1) * QBLOCK)
            keys = slice(start, start + count)
            bias = pair_bias(doc_col, doc_row, q)
            rot, gm = rot_ref[rows], gm_ref[rows]
            dquery = jnp.zeros((QBLOCK, LANES), F32)
            for half in range(2):
                logsum = jnp.sum(
                    jnp.where(lane[rows] == 2 * j + half, lse_ref[rows], 0.0), axis=1, keepdims=True
                )
                scores = nt(rot, spread[half, keys]) * scale + bias
                probs = jnp.exp(scores - logsum)
                dprobs = nt(gm, spread[2 + half, keys])
                inner = jnp.sum(probs * dprobs, axis=1, keepdims=True)
                dscores = (probs * (dprobs - inner)).astype(BF16)
                dquery = dquery + nn(dscores, spread[half, keys])
                dkey[half, keys] += tn(dscores, rot)
                dvalue[half, keys] += tn(probs.astype(BF16), gm)
            out_ref[rows] = turn(dquery * scale, cos_ref[rows], -sin_ref[rows], lane[rows]).astype(BF16)

    @pl.when(j == pairs)
    def _():
        dk = dkey[0] + pltpu.roll(dkey[1], HEAD_DIM, 1)
        dv = pltpu.roll(dvalue[0], HEAD_DIM, 1) + dvalue[1]
        back = turn(dk * scale, cos_ref[...], -sin_ref[...], lane)
        out_ref[...] = jnp.where(lane < HEAD_DIM, back, dv).astype(BF16)


def whole(shape):
    return pl.BlockSpec(shape, lambda j: (0,) * len(shape))


def attend_forward(qkv, doc, cosine, sine, heads):
    length = doc.shape[0]
    pairs = heads * HEAD_DIM // LANES
    column = pl.BlockSpec((length, LANES), lambda j: (0, j))
    return pl.pallas_call(
        lambda *refs: attend_forward_kernel(HEAD_DIM ** (-0.5), *refs),
        grid=(pairs,),
        in_specs=[
            column,
            pl.BlockSpec((length, LANES), lambda j: (0, pairs)),
            whole((length, 1)),
            whole((1, length)),
            whole((length, LANES)),
            whole((length, LANES)),
        ],
        out_specs=[column, column, whole((length, LANES)), whole((length, LANES))],
        out_shape=[
            jax.ShapeDtypeStruct((length, pairs * LANES), BF16),
            jax.ShapeDtypeStruct((length, pairs * LANES), BF16),
            jax.ShapeDtypeStruct((length, LANES), BF16),
            jax.ShapeDtypeStruct((length, LANES), F32),
        ],
        scratch_shapes=[pltpu.VMEM((4, length, LANES), BF16)],
        cost_estimate=pl.CostEstimate(flops=600_000_000, bytes_accessed=4_000_000, transcendentals=1_200_000),
        name="attend_forward",
    )(qkv, qkv, doc.reshape(length, 1), doc.reshape(1, length), cosine, sine)


def attend_backward(rot, kvr, gm, lse, doc, cosine, sine):
    length, width = rot.shape
    pairs = width // LANES
    column = pl.BlockSpec((length, LANES), lambda j: (0, jnp.minimum(j, pairs - 1)))
    return pl.pallas_call(
        lambda *refs: attend_backward_kernel(HEAD_DIM ** (-0.5), pairs, *refs),
        grid=(pairs + 1,),
        in_specs=[
            column,
            whole((length, LANES)),
            column,
            whole((length, LANES)),
            whole((length, 1)),
            whole((1, length)),
            whole((length, LANES)),
            whole((length, LANES)),
        ],
        out_specs=pl.BlockSpec((length, LANES), lambda j: (0, j)),
        out_shape=jax.ShapeDtypeStruct((length, (pairs + 1) * LANES), BF16),
        scratch_shapes=[
            pltpu.VMEM((4, length, LANES), BF16),
            pltpu.VMEM((2, length, LANES), F32),
            pltpu.VMEM((2, length, LANES), F32),
        ],
        cost_estimate=pl.CostEstimate(flops=1_500_000_000, bytes_accessed=4_000_000, transcendentals=1_200_000),
        name="attend_backward",
    )(rot, kvr, gm, lse, doc.reshape(length, 1), doc.reshape(1, length), cosine, sine)


def rms_inverse(residual):
    return lax.rsqrt(jnp.mean(residual * residual, axis=-1, keepdims=True) + EPSILON)


def swap(array, bit):
    return lax.ppermute(array, "dp", [(i, i ^ bit) for i in range(8)])


def at(array, index, axis):
    return lax.dynamic_index_in_dim(array, index, axis, keepdims=False)


class Halving:
    def __init__(self, grad):
        place = lax.axis_index("dp")
        self.core, self.x, self.y = place % 2, place // 2 % 2, place // 4
        rows, width = grad.shape
        self.block = rows // 8
        self.phase = 0
        self.grad = grad.reshape(2, 2, 2, self.block, width)

    def sends(self):
        if self.phase == 0:
            return [(at(self.grad, 1 - self.core, 2), 1)]
        if self.phase == 1:
            return [(at(self.first, 1 - self.x, 1), 2), (at(self.second, 1 - self.y, 0), 4)]
        return [(at(self.first, 1 - self.y, 0), 4), (at(self.second, 1 - self.x, 0), 2)]

    def receive(self, arrays):
        if self.phase == 0:
            total = at(self.grad, self.core, 2) + arrays[0]
            total = total.reshape(2, 2, 2, self.block // 2, total.shape[-1])
            self.first, self.second = total[:, :, 0], total[:, :, 1]
        elif self.phase == 1:
            self.first = at(self.first, self.x, 1) + arrays[0]
            self.second = at(self.second, self.y, 0) + arrays[1]
        else:
            first = at(self.first, self.y, 0).astype(F32) + arrays[0].astype(F32)
            second = at(self.second, self.x, 0).astype(F32) + arrays[1].astype(F32)
            self.total = jnp.concatenate([first, second], axis=0)
        self.phase += 1


class Scatter:
    def __init__(self, grad):
        self.grad = grad
        self.total = None

    def sends(self):
        return []

    def receive(self, arrays):
        if self.total is None:
            self.total = lax.psum_scatter(
                self.grad, "dp", scatter_dimension=0, tiled=True
            ).astype(F32)


def gather_rows(shard):
    rows = shard.shape[0]
    place = lax.axis_index("dp")
    half = rows // 2
    beside, across = swap(shard, 2), swap(shard, 4)
    upper, lower = swap(beside[:half], 4), swap(across[half:], 2)
    four = jnp.concatenate([shard, beside, across, upper, lower], axis=0)
    other = swap(four, 1)
    full = jnp.zeros((8 * rows, shard.shape[1]), shard.dtype)
    for index, bits in enumerate((0, 2, 4, 6)):
        piece = slice(index * rows, (index + 1) * rows)
        full = lax.dynamic_update_slice(full, four[piece], ((place ^ bits) * rows, 0))
        full = lax.dynamic_update_slice(full, other[piece], ((place ^ bits ^ 1) * rows, 0))
    return full


class Line:
    def __init__(self):
        place = lax.axis_index("mp")
        self.end = (place == 0) | (place == 3)
        self.across = self.outward = None
        self.sums = {}

    def step(self, name=None, piece=None, keep=(), others=()):
        arrived = met = back = None
        crossed = [[swap(array, bit) for array, bit in other.sends()] for other in others]
        if name is not None:
            arrived = lax.ppermute(piece, "mp", INWARD)
        if self.across is not None:
            met = lax.ppermute(self.across[1], "mp", ACROSS)
        if self.outward is not None:
            back = lax.ppermute(self.outward[1], "mp", OUTWARD)
        keep, arrived, met, back, crossed = lax.optimization_barrier(
            (keep, arrived, met, back, crossed)
        )
        for other, arrays in zip(others, crossed):
            other.receive(arrays)
        if back is not None:
            self.sums[self.outward[0]] = jnp.where(self.end, back, self.outward[1])
        self.outward = None if met is None else (self.across[0], self.across[1] + met)
        self.across = None if arrived is None else (name, piece + arrived)
        if self.outward is not None or self.across is not None:
            self.outward, self.across = self.rounded(self.outward), self.rounded(self.across)
        return keep

    def rounded(self, entry):
        return None if entry is None else (entry[0], lax.optimization_barrier(entry[1]))


def per_device(
    tokens, doc_ids, selection, w_query, w_key, w_value, w_out, w_gate, w_up, w_down,
    attn_gain, mlp_gain, cotangent,
):
    rows_local, q_width = w_query.shape
    kv_width = w_key.shape[1]
    ff = w_gate.shape[1]
    heads = q_width // HEAD_DIM
    qkv_width = q_width + 2 * kv_width
    seqs, length = doc_ids.shape
    pad = jnp.zeros((rows_local, LANES - 2), BF16)
    front = jnp.concatenate(
        [w_query, w_key, w_value, attn_gain[:, None], mlp_gain[:, None], pad], axis=1
    )
    eight = lax.axis_size("dp") == 8
    if eight:
        front = gather_rows(front)
    else:
        front = lax.all_gather(front, "dp", axis=0, tiled=True)
    w_qkv = front[:, :qkv_width]
    gain_one = front[:, qkv_width].astype(F32)[None, :]
    gain_two = front[:, qkv_width + 1].astype(F32)[None, :]
    full_out = lax.all_gather(w_out, "dp", axis=1, tiled=True)
    full_gate = lax.all_gather(w_gate, "dp", axis=0, tiled=True)
    full_up = lax.all_gather(w_up, "dp", axis=0, tiled=True)
    full_down = lax.all_gather(w_down, "dp", axis=1, tiled=True)

    cosine, sine = rope_tables(length)
    residual = tokens.astype(F32)
    inverse_one = rms_inverse(residual)
    normed_one = (residual * inverse_one * gain_one).astype(BF16)
    grad_y = cotangent.astype(F32) * selection.reshape(-1, 1).astype(F32)
    grad_y_low = grad_y.astype(BF16)

    halves = range(seqs)
    span = [slice(h * length, (h + 1) * length) for h in halves]
    cut = length // 2

    def parts(array):
        return array[:cut], array[cut:]

    line = Line()

    def attention(h):
        qkv = nn(normed_one[span[h]], w_qkv)
        mixed, rot, kvr, lse = attend_forward(qkv, doc_ids[h], cosine, sine, heads)
        partial = nn(mixed, full_out).astype(BF16)
        return mixed, rot, kvr, lse, partial

    def mlp_forward(h):
        attn = jnp.concatenate([line.sums["1", h, 0], line.sums["1", h, 1]], axis=0)
        hidden_in = residual[span[h]] + attn.astype(F32)
        inverse_two = rms_inverse(hidden_in)
        normed_two = (hidden_in * inverse_two * gain_two).astype(BF16)
        gate = nn(normed_two, full_gate)
        up = nn(normed_two, full_up)
        hidden = (gate * jax.nn.sigmoid(gate) * up).astype(BF16)
        partial = nn(hidden, full_down).astype(BF16)
        return attn, normed_two, gate, up, hidden, partial

    def mlp_backward(h, gate, up):
        grad_hidden = nt(grad_y_low[span[h]], full_down)
        sig = jax.nn.sigmoid(gate)
        grad_gate = (grad_hidden * up * sig * (1.0 + gate * (1.0 - sig))).astype(BF16)
        grad_up = (grad_hidden * gate * sig).astype(BF16)
        partial = (nt(grad_gate, full_gate) + nt(grad_up, full_up)).astype(BF16)
        return grad_gate, grad_up, partial

    def attention_backward(h, saved, attn):
        mixed, rot, kvr, lse = saved
        hidden_in = residual[span[h]] + attn.astype(F32)
        inverse_two = rms_inverse(hidden_in)
        grad_normed = jnp.concatenate([line.sums["3", h, 0], line.sums["3", h, 1]], axis=0).astype(F32)
        scaled = grad_normed * gain_two
        gain_part = jnp.sum(grad_normed * hidden_in * inverse_two, axis=0)
        mean_term = jnp.mean(scaled * hidden_in, axis=-1, keepdims=True)
        grad_h = (
            grad_y[span[h]] + inverse_two * scaled - hidden_in * (inverse_two**3) * mean_term
        )
        grad_h_low = grad_h.astype(BF16)
        grad_mixed = nt(grad_h_low, full_out).astype(BF16)
        grad_qkv = attend_backward(rot, kvr, grad_mixed, lse, doc_ids[h], cosine, sine)
        partial = nt(grad_qkv, w_qkv).astype(BF16)
        return grad_h, grad_h_low, grad_qkv, partial, gain_part

    def finish(h, grad_h):
        grad_normed = jnp.concatenate([line.sums["4", h, 0], line.sums["4", h, 1]], axis=0).astype(F32)
        here, inverse = residual[span[h]], inverse_one[span[h]]
        scaled = grad_normed * gain_one
        gain_part = jnp.sum(grad_normed * here * inverse, axis=0)
        mean_term = jnp.mean(scaled * here, axis=-1, keepdims=True)
        return grad_h + inverse * scaled - here * (inverse**3) * mean_term, gain_part

    a = attention(0)
    a_parts = parts(a[4])
    (b,) = line.step(("1", 0, 0), a_parts[0], (attention(1),))
    b_parts = parts(b[4])
    line.step(("1", 0, 1), a_parts[1])
    line.step(("1", 1, 0), b_parts[0])
    line.step(("1", 1, 1), b_parts[1])
    (fa,) = line.step(keep=(mlp_forward(0),))
    attn_a, normed_a, gate_a, up_a, hidden_a, out_a = fa
    out_a = parts(out_a)
    (ba,) = line.step(("2", 0, 0), out_a[0], (mlp_backward(0, gate_a, up_a),))
    gg_a, gu_a, dn_a = ba
    dn_a = parts(dn_a)
    (fb,) = line.step(("3", 0, 0), dn_a[0], (mlp_forward(1),))
    attn_b, normed_b, gate_b, up_b, hidden_b, out_b = fb
    out_b = parts(out_b)
    (bb,) = line.step(("3", 0, 1), dn_a[1], (mlp_backward(1, gate_b, up_b),))
    gg_b, gu_b, dn_b = bb
    dn_b = parts(dn_b)

    def both(first, second):
        return jnp.concatenate([first, second], axis=0)

    normed_two = both(normed_a, normed_b)
    summed = Halving if eight else Scatter
    grad_gate_w, grad_up_w = line.step(
        ("3", 1, 0),
        dn_b[0],
        (tn(normed_two, both(gg_a, gg_b)).astype(BF16), tn(normed_two, both(gu_a, gu_b)).astype(BF16)),
    )
    sum_gate, sum_up = summed(grad_gate_w), summed(grad_up_w)
    (grad_down_w,) = line.step(
        ("3", 1, 1), dn_b[1], (tn(grad_y_low, both(hidden_a, hidden_b)).astype(BF16),), (sum_gate,)
    )
    sum_down = summed(grad_down_w)
    (ca,) = line.step(
        ("2", 0, 1), out_a[1], (attention_backward(0, a[:4], attn_a),), (sum_gate, sum_up)
    )
    gh_a, ghl_a, gq_a, dx_a, gain_two_a = ca
    dx_a = parts(dx_a)
    line.step(("4", 0, 0), dx_a[0], (), (sum_gate, sum_up, sum_down))
    (cb,) = line.step(
        ("4", 0, 1), dx_a[1], (attention_backward(1, b[:4], attn_b),), (sum_up, sum_down)
    )
    gh_b, ghl_b, gq_b, dx_b, gain_two_b = cb
    dx_b = parts(dx_b)
    grad_qkv_w, grad_out_w = line.step(
        ("4", 1, 0),
        dx_b[0],
        (
            tn(normed_one, both(gq_a, gq_b)).astype(BF16),
            tn(both(ghl_a, ghl_b), both(a[0], b[0])).astype(BF16),
        ),
        (sum_down,),
    )
    sum_attn = summed(jnp.concatenate([grad_qkv_w, grad_out_w], axis=1))
    line.step(("4", 1, 1), dx_b[1], (), (sum_attn,))
    (da,) = line.step(("2", 1, 0), out_b[0], (finish(0, gh_a),), (sum_attn,))
    line.step(("2", 1, 1), out_b[1], (), (sum_attn,))
    (db,) = line.step(keep=(finish(1, gh_b),))
    gain_parts = jnp.stack([da[1] + db[1], gain_two_a + gain_two_b]).astype(BF16)
    (gains,) = line.step(
        keep=(lax.psum_scatter(gain_parts, "dp", scatter_dimension=1, tiled=True),)
    )
    gains = gains.astype(F32)

    input_grad = both(da[0], db[0])
    hidden_in = residual + both(attn_a, attn_b).astype(F32)
    mlp_out = jnp.concatenate([line.sums["2", h, i] for h in halves for i in range(2)], axis=0)
    output = (hidden_in + mlp_out.astype(F32)).astype(BF16)
    shard_attn = sum_attn.total
    return (
        output,
        input_grad,
        shard_attn[:, :q_width],
        shard_attn[:, q_width : q_width + kv_width],
        shard_attn[:, q_width + kv_width : qkv_width],
        shard_attn[:, qkv_width:].T,
        sum_gate.total,
        sum_up.total,
        sum_down.total.T,
        gains[0],
        gains[1],
    )


def solution(mesh):
    in_specs = (
        P("dp", None), P("dp", None), P("dp", None), P("dp", "mp"), P("dp", "mp"), P("dp", "mp"),
        P("mp", "dp"), P("dp", "mp"), P("dp", "mp"), P("mp", "dp"), P("dp"), P("dp"), P("dp", None),
    )
    out_specs = (
        P("dp", None), P("dp", None), P("dp", "mp"), P("dp", "mp"), P("dp", "mp"), P("mp", "dp"),
        P("dp", "mp"), P("dp", "mp"), P("mp", "dp"), P("dp"), P("dp"),
    )
    return jax.shard_map(
        per_device, mesh=mesh, in_specs=in_specs, out_specs=out_specs, check_vma=False
    )
```

```python
import jax
import jax.numpy as jnp
from jax import lax
from jax.experimental import pallas as pl
from jax.experimental.pallas import tpu as pltpu
from jax.sharding import PartitionSpec as P

HEAD_DIM = 64
LANES = 128
EPSILON = 1e-05
MASKED = -1e30
QBLOCK = 128
REACH = 256
F32 = jnp.float32
BF16 = jnp.bfloat16

INWARD = [(0, 1), (3, 2)]
ACROSS = [(1, 2), (2, 1)]
OUTWARD = [(1, 0), (2, 3)]


def rope_tables(length):
    half_width = HEAD_DIM // 2
    frequency = 10000.0 ** (-2.0 * jnp.arange(half_width, dtype=F32) / HEAD_DIM)
    places = jnp.arange(length, dtype=F32)
    angles = places[:, None] * frequency[None, :]
    cosine, sine = jnp.cos(angles), jnp.sin(angles)
    return (
        jnp.concatenate([cosine] * 4, axis=1),
        jnp.concatenate([-sine, sine] * 2, axis=1),
    )


def nt(a, b):
    return lax.dot_general(a, b, (((1,), (1,)), ((), ())), preferred_element_type=F32)


def tn(a, b):
    return lax.dot_general(a, b, (((0,), (0,)), ((), ())), preferred_element_type=F32)


def nn(a, b):
    return lax.dot_general(a, b, (((1,), (0,)), ((), ())), preferred_element_type=F32)


def swap_halves(block, lane):
    ahead = pltpu.roll(block, LANES - HEAD_DIM // 2, 1)
    behind = pltpu.roll(block, HEAD_DIM // 2, 1)
    return jnp.where(lane % HEAD_DIM < HEAD_DIM // 2, ahead, behind)


def turn(block, cosine, sine, lane):
    return block * cosine + swap_halves(block, lane) * sine


def key_range(q):
    start = max(0, q * QBLOCK - REACH)
    return start, (q + 1) * QBLOCK - start


def pair_bias(doc_col, doc_row, q):
    start, count = key_range(q)
    rows = lax.broadcasted_iota(jnp.int32, (QBLOCK, count), 0) + q * QBLOCK
    cols = lax.broadcasted_iota(jnp.int32, (QBLOCK, count), 1) + start
    same = doc_col[q * QBLOCK : (q + 1) * QBLOCK, 0:1] == doc_row[0:1, start : start + count]
    return jnp.where(same & (rows >= cols), 0.0, MASKED)


def attend_forward_kernel(
    scale, q_ref, kv_ref, doc_col, doc_row, cos_ref, sin_ref, mixed_ref, rot_ref, kvr_ref, lse_ref, spread
):
    length = q_ref.shape[0]
    j = pl.program_id(0)
    lane = lax.broadcasted_iota(jnp.int32, (length, LANES), 1)

    @pl.when(j == 0)
    def _():
        kv = kv_ref[...]
        turned = turn(kv, cos_ref[...], sin_ref[...], lane)
        kvr_ref[...] = jnp.where(lane < HEAD_DIM, turned, kv).astype(BF16)
        low_key = jnp.where(lane < HEAD_DIM, turned, 0.0)
        high_value = jnp.where(lane < HEAD_DIM, 0.0, kv)
        spread[0] = low_key.astype(BF16)
        spread[1] = pltpu.roll(low_key, HEAD_DIM, 1).astype(BF16)
        spread[2] = pltpu.roll(high_value, HEAD_DIM, 1).astype(BF16)
        spread[3] = high_value.astype(BF16)
        lse_ref[...] = jnp.zeros_like(lse_ref)

    rot = turn(q_ref[...], cos_ref[...], sin_ref[...], lane).astype(BF16)
    rot_ref[...] = rot
    for q in range(length // QBLOCK):
        start, count = key_range(q)
        rows = slice(q * QBLOCK, (q + 1) * QBLOCK)
        keys = slice(start, start + count)
        bias = pair_bias(doc_col, doc_row, q)
        mixed = jnp.zeros((QBLOCK, LANES), F32)
        for half in range(2):
            scores = nt(rot[rows], spread[half, keys]) * scale + bias
            highest = jnp.max(scores, axis=1, keepdims=True)
            raised = jnp.exp(scores - highest)
            total = jnp.sum(raised, axis=1, keepdims=True)
            probs = (raised * (1.0 / total)).astype(BF16)
            mixed = mixed + nn(probs, spread[2 + half, keys])
            lse_ref[rows] = jnp.where(
                lane[rows] == 2 * j + half, highest + jnp.log(total), lse_ref[rows]
            )
        mixed_ref[rows] = mixed.astype(BF16)


def attend_backward_kernel(
    scale, pairs, rot_ref, kvr_ref, gm_ref, lse_ref, doc_col, doc_row, cos_ref, sin_ref, out_ref, spread, dkey, dvalue
):
    length = rot_ref.shape[0]
    j = pl.program_id(0)
    lane = lax.broadcasted_iota(jnp.int32, (length, LANES), 1)

    @pl.when(j == 0)
    def _():
        kvr = kvr_ref[...].astype(F32)
        low_key = jnp.where(lane < HEAD_DIM, kvr, 0.0)
        high_value = jnp.where(lane < HEAD_DIM, 0.0, kvr)
        spread[0] = low_key.astype(BF16)
        spread[1] = pltpu.roll(low_key, HEAD_DIM, 1).astype(BF16)
        spread[2] = pltpu.roll(high_value, HEAD_DIM, 1).astype(BF16)
        spread[3] = high_value.astype(BF16)
        dkey[...] = jnp.zeros_like(dkey)
        dvalue[...] = jnp.zeros_like(dvalue)

    @pl.when(j < pairs)
    def _():
        for q in range(length // QBLOCK):
            start, count = key_range(q)
            rows = slice(q * QBLOCK, (q + 1) * QBLOCK)
            keys = slice(start, start + count)
            bias = pair_bias(doc_col, doc_row, q)
            rot, gm = rot_ref[rows], gm_ref[rows]
            dquery = jnp.zeros((QBLOCK, LANES), F32)
            for half in range(2):
                logsum = jnp.sum(
                    jnp.where(lane[rows] == 2 * j + half, lse_ref[rows], 0.0), axis=1, keepdims=True
                )
                scores = nt(rot, spread[half, keys]) * scale + bias
                probs = jnp.exp(scores - logsum)
                dprobs = nt(gm, spread[2 + half, keys])
                inner = jnp.sum(probs * dprobs, axis=1, keepdims=True)
                dscores = (probs * (dprobs - inner)).astype(BF16)
                dquery = dquery + nn(dscores, spread[half, keys])
                dkey[half, keys] += tn(dscores, rot)
                dvalue[half, keys] += tn(probs.astype(BF16), gm)
            out_ref[rows] = turn(dquery * scale, cos_ref[rows], -sin_ref[rows], lane[rows]).astype(BF16)

    @pl.when(j == pairs)
    def _():
        dk = dkey[0] + pltpu.roll(dkey[1], HEAD_DIM, 1)
        dv = pltpu.roll(dvalue[0], HEAD_DIM, 1) + dvalue[1]
        back = turn(dk * scale, cos_ref[...], -sin_ref[...], lane)
        out_ref[...] = jnp.where(lane < HEAD_DIM, back, dv).astype(BF16)


def whole(shape):
    return pl.BlockSpec(shape, lambda j: (0,) * len(shape))


def attend_forward(qkv, doc, cosine, sine, heads):
    length = doc.shape[0]
    pairs = heads * HEAD_DIM // LANES
    column = pl.BlockSpec((length, LANES), lambda j: (0, j))
    return pl.pallas_call(
        lambda *refs: attend_forward_kernel(HEAD_DIM ** (-0.5), *refs),
        grid=(pairs,),
        in_specs=[
            column,
            pl.BlockSpec((length, LANES), lambda j: (0, pairs)),
            whole((length, 1)),
            whole((1, length)),
            whole((length, LANES)),
            whole((length, LANES)),
        ],
        out_specs=[column, column, whole((length, LANES)), whole((length, LANES))],
        out_shape=[
            jax.ShapeDtypeStruct((length, pairs * LANES), BF16),
            jax.ShapeDtypeStruct((length, pairs * LANES), BF16),
            jax.ShapeDtypeStruct((length, LANES), BF16),
            jax.ShapeDtypeStruct((length, LANES), F32),
        ],
        scratch_shapes=[pltpu.VMEM((4, length, LANES), BF16)],
        cost_estimate=pl.CostEstimate(flops=600_000_000, bytes_accessed=4_000_000, transcendentals=1_200_000),
        name="attend_forward",
    )(qkv, qkv, doc.reshape(length, 1), doc.reshape(1, length), cosine, sine)


def attend_backward(rot, kvr, gm, lse, doc, cosine, sine):
    length, width = rot.shape
    pairs = width // LANES
    column = pl.BlockSpec((length, LANES), lambda j: (0, jnp.minimum(j, pairs - 1)))
    return pl.pallas_call(
        lambda *refs: attend_backward_kernel(HEAD_DIM ** (-0.5), pairs, *refs),
        grid=(pairs + 1,),
        in_specs=[
            column,
            whole((length, LANES)),
            column,
            whole((length, LANES)),
            whole((length, 1)),
            whole((1, length)),
            whole((length, LANES)),
            whole((length, LANES)),
        ],
        out_specs=pl.BlockSpec((length, LANES), lambda j: (0, j)),
        out_shape=jax.ShapeDtypeStruct((length, (pairs + 1) * LANES), BF16),
        scratch_shapes=[
            pltpu.VMEM((4, length, LANES), BF16),
            pltpu.VMEM((2, length, LANES), F32),
            pltpu.VMEM((2, length, LANES), F32),
        ],
        cost_estimate=pl.CostEstimate(flops=1_500_000_000, bytes_accessed=4_000_000, transcendentals=1_200_000),
        name="attend_backward",
    )(rot, kvr, gm, lse, doc.reshape(length, 1), doc.reshape(1, length), cosine, sine)


def rms_inverse(residual):
    return lax.rsqrt(jnp.mean(residual * residual, axis=-1, keepdims=True) + EPSILON)


class Line:
    def __init__(self):
        place = lax.axis_index("mp")
        self.end = (place == 0) | (place == 3)
        self.across = self.outward = None
        self.sums = {}

    def step(self, name=None, piece=None, keep=()):
        arrived = met = back = None
        if name is not None:
            arrived = lax.ppermute(piece, "mp", INWARD)
        if self.across is not None:
            met = lax.ppermute(self.across[1], "mp", ACROSS)
        if self.outward is not None:
            back = lax.ppermute(self.outward[1], "mp", OUTWARD)
        keep, arrived, met, back = lax.optimization_barrier((keep, arrived, met, back))
        if back is not None:
            self.sums[self.outward[0]] = jnp.where(self.end, back, self.outward[1])
        self.outward = None if met is None else (self.across[0], self.across[1] + met)
        self.across = None if arrived is None else (name, piece + arrived)
        if self.outward is not None or self.across is not None:
            self.outward, self.across = self.rounded(self.outward), self.rounded(self.across)
        return keep

    def rounded(self, entry):
        return None if entry is None else (entry[0], lax.optimization_barrier(entry[1]))


def per_device(
    tokens, doc_ids, selection, w_query, w_key, w_value, w_out, w_gate, w_up, w_down,
    attn_gain, mlp_gain, cotangent,
):
    rows_local, q_width = w_query.shape
    kv_width = w_key.shape[1]
    heads = q_width // HEAD_DIM
    qkv_width = q_width + 2 * kv_width
    seqs, length = doc_ids.shape
    pad = jnp.zeros((rows_local, LANES - 2), BF16)
    front = jnp.concatenate(
        [w_query, w_key, w_value, attn_gain[:, None], mlp_gain[:, None], pad], axis=1
    )
    front = lax.all_gather(front, "dp", axis=0, tiled=True)
    w_qkv = front[:, :qkv_width]
    gain_one = front[:, qkv_width].astype(F32)[None, :]
    gain_two = front[:, qkv_width + 1].astype(F32)[None, :]
    full_out = lax.all_gather(w_out, "dp", axis=1, tiled=True)
    full_gate = lax.all_gather(w_gate, "dp", axis=0, tiled=True)
    full_up = lax.all_gather(w_up, "dp", axis=0, tiled=True)
    full_down = lax.all_gather(w_down, "dp", axis=1, tiled=True)

    cosine, sine = rope_tables(length)
    residual = tokens.astype(F32)
    inverse_one = rms_inverse(residual)
    normed_one = (residual * inverse_one * gain_one).astype(BF16)
    grad_y = cotangent.astype(F32) * selection.reshape(-1, 1).astype(F32)
    grad_y_low = grad_y.astype(BF16)

    halves = range(seqs)
    span = [slice(h * length, (h + 1) * length) for h in halves]
    cut = length // 2

    def parts(array):
        return array[:cut], array[cut:]

    line = Line()

    def attention(h):
        qkv = nn(normed_one[span[h]], w_qkv)
        mixed, rot, kvr, lse = attend_forward(qkv, doc_ids[h], cosine, sine, heads)
        partial = nn(mixed, full_out).astype(BF16)
        return mixed, rot, kvr, lse, partial

    def mlp_forward(h):
        attn = jnp.concatenate([line.sums["1", h, 0], line.sums["1", h, 1]], axis=0)
        hidden_in = residual[span[h]] + attn.astype(F32)
        inverse_two = rms_inverse(hidden_in)
        normed_two = (hidden_in * inverse_two * gain_two).astype(BF16)
        gate = nn(normed_two, full_gate)
        up = nn(normed_two, full_up)
        hidden = (gate * jax.nn.sigmoid(gate) * up).astype(BF16)
        partial = nn(hidden, full_down).astype(BF16)
        return attn, normed_two, gate, up, hidden, partial

    def mlp_backward(h, gate, up):
        grad_hidden = nt(grad_y_low[span[h]], full_down)
        sig = jax.nn.sigmoid(gate)
        grad_gate = (grad_hidden * up * sig * (1.0 + gate * (1.0 - sig))).astype(BF16)
        grad_up = (grad_hidden * gate * sig).astype(BF16)
        partial = (nt(grad_gate, full_gate) + nt(grad_up, full_up)).astype(BF16)
        return grad_gate, grad_up, partial

    def attention_backward(h, saved, attn):
        _, rot, kvr, lse = saved
        hidden_in = residual[span[h]] + attn.astype(F32)
        inverse_two = rms_inverse(hidden_in)
        grad_normed = jnp.concatenate([line.sums["3", h, 0], line.sums["3", h, 1]], axis=0).astype(F32)
        scaled = grad_normed * gain_two
        gain_part = jnp.sum(grad_normed * hidden_in * inverse_two, axis=0)
        mean_term = jnp.mean(scaled * hidden_in, axis=-1, keepdims=True)
        grad_h = (
            grad_y[span[h]] + inverse_two * scaled - hidden_in * (inverse_two**3) * mean_term
        )
        grad_h_low = grad_h.astype(BF16)
        grad_mixed = nt(grad_h_low, full_out).astype(BF16)
        grad_qkv = attend_backward(rot, kvr, grad_mixed, lse, doc_ids[h], cosine, sine)
        partial = nt(grad_qkv, w_qkv).astype(BF16)
        return grad_h, grad_h_low, grad_qkv, partial, gain_part

    def finish(h, grad_h):
        grad_normed = jnp.concatenate([line.sums["4", h, 0], line.sums["4", h, 1]], axis=0).astype(F32)
        here, inverse = residual[span[h]], inverse_one[span[h]]
        scaled = grad_normed * gain_one
        gain_part = jnp.sum(grad_normed * here * inverse, axis=0)
        mean_term = jnp.mean(scaled * here, axis=-1, keepdims=True)
        return grad_h + inverse * scaled - here * (inverse**3) * mean_term, gain_part

    def scatter(grad, axis):
        total = lax.psum_scatter(grad, "dp", scatter_dimension=axis, tiled=True)
        return total.astype(F32)

    a = attention(0)
    a_parts = parts(a[4])
    (b,) = line.step(("1", 0, 0), a_parts[0], (attention(1),))
    b_parts = parts(b[4])
    line.step(("1", 0, 1), a_parts[1])
    line.step(("1", 1, 0), b_parts[0])
    line.step(("1", 1, 1), b_parts[1])
    (fa,) = line.step(keep=(mlp_forward(0),))
    attn_a, normed_a, gate_a, up_a, hidden_a, out_a = fa
    out_a = parts(out_a)
    (ba,) = line.step(("2", 0, 0), out_a[0], (mlp_backward(0, gate_a, up_a),))
    gg_a, gu_a, dn_a = ba
    dn_a = parts(dn_a)
    (fb,) = line.step(("3", 0, 0), dn_a[0], (mlp_forward(1),))
    attn_b, normed_b, gate_b, up_b, hidden_b, out_b = fb
    out_b = parts(out_b)
    (bb,) = line.step(("3", 0, 1), dn_a[1], (mlp_backward(1, gate_b, up_b),))
    gg_b, gu_b, dn_b = bb
    dn_b = parts(dn_b)

    def both(first, second):
        return jnp.concatenate([first, second], axis=0)

    normed_two = both(normed_a, normed_b)
    (grad_gate_w, grad_up_w) = line.step(
        ("3", 1, 0),
        dn_b[0],
        (tn(normed_two, both(gg_a, gg_b)).astype(BF16), tn(normed_two, both(gu_a, gu_b)).astype(BF16)),
    )
    (grad_down_w,) = line.step(
        ("3", 1, 1), dn_b[1], (tn(both(hidden_a, hidden_b), grad_y_low).astype(BF16),)
    )
    (ca,) = line.step(("2", 0, 1), out_a[1], (attention_backward(0, a[:4], attn_a),))
    gh_a, ghl_a, gq_a, dx_a, gain_two_a = ca
    dx_a = parts(dx_a)
    line.step(("4", 0, 0), dx_a[0])
    (cb,) = line.step(("4", 0, 1), dx_a[1], (attention_backward(1, b[:4], attn_b),))
    gh_b, ghl_b, gq_b, dx_b, gain_two_b = cb
    dx_b = parts(dx_b)
    grad_qkv_w, grad_out_w = line.step(
        ("4", 1, 0),
        dx_b[0],
        (
            tn(normed_one, both(gq_a, gq_b)).astype(BF16),
            tn(both(a[0], b[0]), both(ghl_a, ghl_b)).astype(BF16),
        ),
    )
    line.step(("4", 1, 1), dx_b[1])
    (da,) = line.step(("2", 1, 0), out_b[0], (finish(0, gh_a),))
    line.step(("2", 1, 1), out_b[1])
    (db,) = line.step(keep=(finish(1, gh_b),))
    line.step()

    input_grad = both(da[0], db[0])
    hidden_in = residual + both(attn_a, attn_b).astype(F32)
    mlp_out = jnp.concatenate([line.sums["2", h, i] for h in halves for i in range(2)], axis=0)
    output = (hidden_in + mlp_out.astype(F32)).astype(BF16)
    shard_gate = scatter(grad_gate_w, 0)
    shard_up = scatter(grad_up_w, 0)
    shard_down = scatter(grad_down_w, 1)
    shard_qkv = scatter(grad_qkv_w, 0)
    shard_out = scatter(grad_out_w, 1)
    return (
        output,
        input_grad,
        shard_qkv[:, :q_width],
        shard_qkv[:, q_width : q_width + kv_width],
        shard_qkv[:, q_width + kv_width :],
        shard_out,
        shard_gate,
        shard_up,
        shard_down,
        scatter((da[1] + db[1]).astype(BF16), 0),
        scatter((gain_two_a + gain_two_b).astype(BF16), 0),
    )


def solution(mesh):
    in_specs = (
        P("dp", None), P("dp", None), P("dp", None), P("dp", "mp"), P("dp", "mp"), P("dp", "mp"),
        P("mp", "dp"), P("dp", "mp"), P("dp", "mp"), P("mp", "dp"), P("dp"), P("dp"), P("dp", None),
    )
    out_specs = (
        P("dp", None), P("dp", None), P("dp", "mp"), P("dp", "mp"), P("dp", "mp"), P("mp", "dp"),
        P("dp", "mp"), P("dp", "mp"), P("mp", "dp"), P("dp"), P("dp"),
    )

    return jax.shard_map(
        per_device, mesh=mesh, in_specs=in_specs, out_specs=out_specs, check_vma=False
    )
```
